512 devices in a mesh: seq: 128 (over y, z, core), head: 4 (over x).
Axes of the slice: x: 4, y: 8, z: 8, core: 2. Of those that a mesh axis runs over, the one named last changes fastest.
Arguments:
- seq_inputs: bfloat16 [1, 32768, 4096], P(None, 'seq', 'head'), may hold values from -6 to 6
- gate_inputs: bfloat16 [1, 32768, 4096], P(None, 'seq', 'head'), may hold values from -6 to 6
- projections: bfloat16 [1, 32768, 256], P(None, 'seq'), may hold values from -6 to 6
- step_raw: float32 [1, 32768, 64], P(None, 'seq', 'head'), may hold values from -3 to 3
- step_bias: float32 [64], P('head'), may hold values from -1 to 1
- decay_rate: float32 [64], P('head'), may hold values from 3.0517578e-05 to 8
- conv_feature: float32 [4, 4096], P(None, 'head'), may hold values from -3 to 3
- conv_proj: float32 [4, 256], replicated, may hold values from -3 to 3
- norm_gain: float32 [4096], P('head'), may hold values from 0.25 to 1.75
Outputs:
- mixed_out: bfloat16 [1, 32768, 4096], P(None, 'seq', 'head')
The draws below stay inside these ranges and needn't reach their ends.
All inputs are finite; a program needn't handle non-finite values.
Results may differ from the reference program's by a relative error of at most 0.0034.
Values may be sent and summed in bfloat16 or wider, within the bound.
No kernel may reach another device: no remote copies, remote signals or barrier semaphores. Data moves between devices by JAX's collectives and lax.ppermute only.
A program may use at most 192 MiB of HBM per device.

```python
import math
import jax
import jax.numpy as jnp
from jax import lax

HEADS = 64
HEAD_DIM = 64
STATE = 128
CONV = 4
STRETCH = 256
BATCH = 1
TOKENS = 32768


def block_scale(own_key, shape, pieces, low, largest):
    def one(position, parts):
        draws = jax.random.uniform(jax.random.fold_in(jax.random.fold_in(own_key, 6), position), (parts,), jnp.float32, low / len(pieces), largest / len(pieces))
        return jnp.repeat(jnp.exp(draws), shape[position] // parts).reshape((-1,) + (1,) * (len(shape) - position - 1))

    gain = one(*pieces[0])
    for cut in pieces[1:]:
        gain = gain * one(*cut)
    return gain


def centred(stream_key, shape, width, limit, split=(), kind=jnp.bfloat16):
    result = width * jax.random.normal(stream_key, shape, jnp.float32)
    if split:
        result = result * block_scale(stream_key, shape, split, -0.22, 0.18)
    return jnp.clip(result, -limit, limit).astype(kind)


def setup_inputs(seed: int = 0) -> dict:
    streams_of = jax.random.split(jax.random.key(seed), 10)
    return {
        "seq_inputs": centred(streams_of[0], (BATCH, TOKENS, HEADS * HEAD_DIM), 1.0, 6.0, ((1, 128), (2, 4))),
        "gate_inputs": centred(streams_of[1], (BATCH, TOKENS, HEADS * HEAD_DIM), 1.0, 6.0, ((1, 128), (2, 4))),
        "projections": centred(streams_of[2], (BATCH, TOKENS, 2 * STATE), 1.0, 6.0, ((1, 128),)),
        "step_raw": centred(streams_of[3], (BATCH, TOKENS, HEADS), 0.5, 3.0, ((1, 128), (2, 4)), jnp.float32),
        "step_bias": jnp.clip(jax.random.uniform(streams_of[4], (HEADS,), jnp.float32, -1.0, 1.0) * block_scale(streams_of[4], (HEADS,), ((0, 4),), -0.4, 0.0), -1.0, 1.0),
        "decay_rate": jnp.clip(jnp.exp(math.log(8.0) - 12.476649 * jax.random.uniform(streams_of[5], (HEADS,), jnp.float32) ** block_scale(streams_of[5], (HEADS,), ((0, 4),), -0.2, 0.2)), 3.0517578125e-05, 8.0),
        "conv_feature": centred(streams_of[6], (CONV, HEADS * HEAD_DIM), CONV ** -0.5, 3.0, ((1, 4),), jnp.float32),
        "conv_proj": centred(streams_of[7], (CONV, 2 * STATE), CONV ** -0.5, 3.0, (), jnp.float32),
        "norm_gain": jnp.clip(1.0 + 0.15 * jax.random.normal(streams_of[8], (HEADS * HEAD_DIM,), jnp.float32), 0.25, 1.75),
    }


def settle(values):
    return lax.optimization_barrier(values.astype(jnp.bfloat16)).astype(jnp.float32)

def causal_mix(window, weights):
    kernel_len = weights.shape[0]
    length = window.shape[1] - kernel_len + 1
    running = window[:, 0:length].astype(jnp.float32) * weights[0]
    for offset in range(1, kernel_len):
        running = running + window[:, offset:offset + length].astype(jnp.float32) * weights[offset]
    return settle(jax.nn.silu(running))

def block_terms(x_mixed, write_vec, read_vec, step_size, decay_rate, carried):
    log_decay = jnp.cumsum(step_size * -decay_rate, axis=1)
    scores = jnp.einsum('btn,bsn->bts', read_vec, write_vec)
    causal = jnp.arange(STRETCH)[:, None] >= jnp.arange(STRETCH)[None, :]
    decay_gap = jnp.where(causal[None, :, :, None], log_decay[:, :, None, :] - log_decay[:, None, :, :], 0.0)
    mixing = settle(jnp.where(causal[None, :, :, None], scores[:, :, :, None] * jnp.exp(decay_gap) * step_size[:, None, :, :], 0.0))
    within = jnp.einsum('btsh,bshp->bthp', mixing, x_mixed)
    to_end = jnp.exp(log_decay[:, -1:, :] - log_decay) * step_size
    weighted = settle(x_mixed * to_end[:, :, :, None])
    summary = jnp.einsum('bshp,bsn->bhpn', weighted, write_vec)
    outside = jnp.einsum('bhpn,btn->bthp', settle(carried), read_vec) * jnp.exp(log_decay)[:, :, :, None]
    next_carried = jnp.exp(log_decay[:, -1, :])[:, :, None, None] * carried + summary
    return (within + outside, next_carried)

def reference(seq_inputs, gate_inputs, projections, step_raw, step_bias, decay_rate, conv_feature, conv_proj, norm_gain):
    kernel_len = conv_feature.shape[0]
    padded_x = jnp.pad(seq_inputs, ((0, 0), (kernel_len - 1, 0), (0, 0)))
    padded_proj = jnp.pad(projections, ((0, 0), (kernel_len - 1, 0), (0, 0)))

    def advance(carried, block_id):
        start = (block_id * STRETCH).astype(jnp.int32)
        window_x = lax.dynamic_slice_in_dim(padded_x, start, STRETCH + kernel_len - 1, 1)
        window_proj = lax.dynamic_slice_in_dim(padded_proj, start, STRETCH + kernel_len - 1, 1)
        x_mixed = causal_mix(window_x, conv_feature).reshape(BATCH, STRETCH, HEADS, HEAD_DIM)
        proj_mixed = causal_mix(window_proj, conv_proj)
        write_vec = proj_mixed[:, :, :STATE]
        read_vec = proj_mixed[:, :, STATE:]
        step_size = jax.nn.softplus(lax.dynamic_slice_in_dim(step_raw, start, STRETCH, 1) + step_bias)
        outputs, carried = block_terms(x_mixed, write_vec, read_vec, step_size, decay_rate, carried)
        gate_block = lax.dynamic_slice_in_dim(gate_inputs, start, STRETCH, 1)
        gated = outputs.reshape(BATCH, STRETCH, HEADS * HEAD_DIM) * jax.nn.silu(gate_block.astype(jnp.float32))
        scale = lax.rsqrt(lax.optimization_barrier(jnp.mean(gated * gated, axis=-1)) + 1.0)
        return (carried, (gated * scale[:, :, None] * norm_gain).astype(jnp.bfloat16))
    initial = jnp.zeros((BATCH, HEADS, HEAD_DIM, STATE), jnp.float32)
    _, stacked = lax.scan(advance, initial, jnp.arange(TOKENS // STRETCH, dtype=jnp.int32))
    return jnp.transpose(stacked, (1, 0, 2, 3)).reshape(BATCH, TOKENS, HEADS * HEAD_DIM)
```

```python
import jax
import jax.numpy as jnp
from jax import lax
from jax.experimental import pallas as pl
from jax.experimental.pallas import tpu as pltpu
from jax.sharding import Mesh, PartitionSpec as P

HEADS = 64
HEAD_DIM = 64
TOKENS_LOCAL = 256
CHANNELS = 1024
HALF = 512
STATE = 128
HEADS_LOCAL = 16
CHIPS = 64
LOG2E = 1.4426950408889634
F32 = jnp.float32
BF16 = jnp.bfloat16


def silu(value):
    half = 0.5 * value
    return half + half * jnp.tanh(half)


def parts_of(value):
    high = value.astype(BF16)
    rest = value - high.astype(F32)
    middle = rest.astype(BF16)
    low = (rest - middle.astype(F32)).astype(BF16)
    return high, middle, low


def dot(left, right, dims=((1,), (0,))):
    return lax.dot_general(left, right, (dims, ((), ())), preferred_element_type=F32)


def conv_silu(values, taps):
    values = values.astype(F32)
    running = values * taps[0:1]
    for k in range(1, 4):
        running = pltpu.roll(running, 1, 0) + values * taps[k : k + 1]
    return silu(running).astype(BF16)


def conv_first(ext_ref, taps, width):
    at = slice(0, width)
    running = ext_ref[5:13, at] * taps[0:1]
    for k in range(1, 4):
        running = running + ext_ref[5 + k : 13 + k, at] * taps[k : k + 1]
    return silu(running).astype(BF16)


def copy_all(pairs, sems):
    copies = [
        pltpu.make_async_copy(source, target, sems.at[place])
        for place, (source, target) in enumerate(pairs)
    ]
    for copy in copies:
        copy.start()
    return copies


def column_of(row):
    first = lax.broadcasted_iota(jnp.int32, (HEADS_LOCAL, HEADS_LOCAL), 0)
    second = lax.broadcasted_iota(jnp.int32, (HEADS_LOCAL, HEADS_LOCAL), 1)
    return jnp.sum(jnp.where(first == second, row, 0.0), axis=1, keepdims=True)


def prepare(
    x_ref, proj_ref, step_ref, bias_ref, rate_ref, tapx_ref, tapp_ref,
    step_out_ref, log_rows_ref, log_columns_ref, factor_ref, now_ref,
    near_x, near_proj, to_end_ref, end_ref, near_tapx, near_tapp,
    near_step, near_bias, near_rate, sems, tail_ref=None,
):
    pairs = [(step_ref, near_step), (bias_ref, near_bias), (rate_ref, near_rate)]
    if tail_ref is not None:
        rows = pl.ds(TOKENS_LOCAL - 8, 8)
        pairs += [
            (x_ref.at[rows], tail_ref.at[:, pl.ds(0, CHANNELS)]),
            (proj_ref.at[rows], tail_ref.at[:, pl.ds(CHANNELS, 2 * STATE)]),
        ]
    pairs += [
        (proj_ref, near_proj),
        (x_ref, near_x),
        (tapx_ref, near_tapx),
        (tapp_ref, near_tapp),
    ]
    copies = copy_all(pairs, sems)
    row = lax.broadcasted_iota(jnp.int32, (TOKENS_LOCAL, TOKENS_LOCAL), 0)
    col = lax.broadcasted_iota(jnp.int32, (TOKENS_LOCAL, TOKENS_LOCAL), 1)
    upper = (row <= col).astype(BF16)
    head = lax.broadcasted_iota(jnp.int32, (3 * HEADS_LOCAL, CHANNELS), 0)
    channel = lax.broadcasted_iota(jnp.int32, (3 * HEADS_LOCAL, CHANNELS), 1)
    spread = (channel // HEAD_DIM == head % HEADS_LOCAL).astype(BF16)

    def stacked(value):
        return jnp.concatenate(parts_of(value), axis=0)

    def to_channels(value):
        return dot(stacked(value), spread, ((0,), (0,)))

    for copy in copies[:3]:
        copy.wait()
    raw = near_step[...] + column_of(near_bias[...])
    step = jnp.maximum(raw, 0.0) + jnp.log1p(jnp.exp(-jnp.abs(raw)))
    sums = dot(stacked(step * -column_of(near_rate[...])), upper)
    log_decay = sums[:HEADS_LOCAL] + sums[HEADS_LOCAL : 2 * HEADS_LOCAL] + sums[2 * HEADS_LOCAL :]
    step_out_ref[...] = step
    log2 = log_decay * LOG2E
    log_rows_ref[...] = log2
    pad = jnp.zeros((128 - HEADS_LOCAL, TOKENS_LOCAL), F32)
    log_columns_ref[...] = jnp.transpose(jnp.concatenate([log2, pad], axis=0))
    last = log_decay[:, TOKENS_LOCAL - 1 :]
    to_end_ref[...] = to_channels(jnp.exp(last - log_decay) * step)
    factor_ref[...] = to_channels(jnp.broadcast_to(jnp.exp(last), (HEADS_LOCAL, 8)))
    now_ref[...] = to_channels(jnp.exp(log_decay))
    token = lax.broadcasted_iota(jnp.int32, (8, 1), 0)
    end_ref[...] = jnp.where(token < 3, to_end_ref[:8], 0.0)
    to_end_ref[:8] = jnp.where(token < 3, 0.0, to_end_ref[:8])
    for copy in copies[3:]:
        copy.wait()


def early_kernel(*refs):
    inputs, tail_ref, rest = refs[:7], refs[7], refs[8:]

    @pl.when(lax.axis_index("core") == 1)
    def _():
        prepare(*inputs, *rest, tail_ref=tail_ref)


def state_kernel(*refs):
    inputs, rest = refs[:7], refs[18:]
    outputs, (xm_ref, pm_ref, sums_ref, send_ref), scratch = rest[:11], rest[11:15], rest[15:]
    factor_ref = outputs[3]
    near_x, near_proj, to_end_ref, end_ref, tapx_ref, tapp_ref = outputs[5:11]
    core = lax.axis_index("core")

    @pl.when(core == 0)
    def _():
        prepare(*inputs, *outputs, *scratch)

    is_first = first_core()
    pm = conv_silu(near_proj[...], tapp_ref[...])
    pm_ref[...] = pm
    turned = jnp.transpose(pm[:, :STATE].astype(F32)).astype(BF16)
    width = 256
    for tile in range(CHANNELS // width):
        at = slice(tile * width, (tile + 1) * width)
        xm = conv_silu(near_x[:, at], tapx_ref[:, at])
        xm_ref[:, at] = xm
        weighted = (xm.astype(F32) * to_end_ref[:, at]).astype(BF16)
        half, inside = divmod(tile * width, HALF)
        sums_ref[half, :STATE, inside : inside + width] = dot(turned, weighted)
    head_x = near_x[:8].astype(F32)
    head_proj = near_proj[:8].astype(F32)
    tail_x = near_x[-8:].astype(F32)
    tail_proj = near_proj[-8:].astype(F32)
    for half in range(2):
        at = slice(half * HALF, (half + 1) * HALF)
        sums_ref[half, STATE : STATE + 8] = factor_ref[:, at]
        sums_ref[half, STATE + 8 : STATE + 16] = jnp.where(
            is_first, tail_x[:, :HALF], head_x[:, at]
        )
        sums_ref[half, STATE + 16 : STATE + 24] = jnp.where(
            is_first, tail_x[:, HALF:], end_ref[:, at]
        )
        sums_ref[half, STATE + 24 :, : 2 * STATE] = jnp.where(is_first, tail_proj, head_proj)
        sums_ref[half, STATE + 24 :, 2 * STATE :] = jnp.zeros((8, HALF - 2 * STATE), F32)
    send_ref[...] = sums_ref[1 - core]


def first_of(halo_x, halo_proj, head_x, head_proj, tapx, tapp, ext_ref, extp_ref):
    width = halo_x.shape[1]
    ext_ref[:8] = halo_x
    ext_ref[8:] = head_x
    extp_ref[:8] = halo_proj
    extp_ref[8:] = head_proj
    pm = conv_first(extp_ref, tapp, 2 * STATE)
    return conv_first(ext_ref, tapx, width), pm


def first_core():
    return jnp.full((1, 1), lax.axis_index("core"), jnp.int32) == 0


def first_kernel(
    halo_ref, x_ref, proj_ref, end_ref, tapx_ref, tapp_ref, own_ref, send_ref, ext_ref, extp_ref
):
    halo = halo_ref[...].astype(F32)
    xm, pm = first_of(
        halo[:, :CHANNELS], halo[:, CHANNELS:], x_ref[:8].astype(F32), proj_ref[:8].astype(F32),
        tapx_ref[...], tapp_ref[...], ext_ref, extp_ref,
    )
    weighted = (xm.astype(F32) * end_ref[...]).astype(BF16)
    own_ref[:, :HALF] = weighted[:, :HALF]
    own_ref[:, HALF:] = pm[:, :STATE]
    send_ref[:, :HALF] = weighted[:, HALF:]
    send_ref[:, HALF:] = pm[:, :STATE]


def join_kernel(
    sums_ref, recv_ref, x_ref, proj_ref, tapx_ref, tapp_ref, own_rows_ref, recv_rows_ref,
    message_ref, first_ref, ext_ref, extp_ref,
):
    core = lax.axis_index("core")
    is_first = first_core()
    own = sums_ref[core]
    other = recv_ref[...]
    tail_x = x_ref[-8:].astype(F32)
    tail_proj = proj_ref[-8:].astype(F32)
    taps = tapx_ref[...]
    xm, pm = first_of(
        jnp.where(is_first, tail_x[:, :HALF], other[STATE + 16 : STATE + 24]),
        jnp.where(is_first, tail_proj, other[STATE + 24 :, : 2 * STATE]),
        jnp.where(is_first, other[STATE + 8 : STATE + 16], own[STATE + 8 : STATE + 16]),
        jnp.where(is_first, other[STATE + 24 :, : 2 * STATE], own[STATE + 24 :, : 2 * STATE]),
        jnp.where(is_first, taps[:, :HALF], taps[:, HALF:]),
        tapp_ref[...],
        ext_ref,
        extp_ref,
    )
    end = jnp.where(is_first, other[STATE + 16 : STATE + 24], own[STATE + 16 : STATE + 24])
    added = dot(pm[:, :STATE], (xm.astype(F32) * end).astype(BF16), ((0,), (0,)))
    rows = jnp.where(
        is_first, own_rows_ref[...].astype(F32), recv_rows_ref[...].astype(F32)
    ).astype(BF16)
    added_first = dot(rows[:, HALF:], rows[:, :HALF], ((0,), (0,)))
    first = jnp.where(is_first, own[: STATE + 8], other[: STATE + 8])
    second = jnp.where(is_first, other[: STATE + 8], own[: STATE + 8])
    first_state = first[:STATE] + added_first
    first_ref[:STATE] = first_state
    first_ref[STATE:] = first[STATE:]
    factor = second[STATE:] * first[STATE:]
    total = second[STATE : STATE + 1] * first_state + (second[:STATE] + added)
    high = factor.astype(BF16)
    low = (factor - high.astype(F32)).astype(BF16)
    row = lax.broadcasted_iota(jnp.int32, (8, HALF), 0)
    tags = jnp.where(row == 0, high.astype(F32), low.astype(F32)).astype(BF16)
    total = total.astype(BF16)
    for group in range(STATE // 8):
        for lane in range(HALF // 128):
            at = slice(lane * 128, (lane + 1) * 128)
            slot = group * (HALF // 128) + lane
            for piece in range(4):
                start = group * 8 + piece * 2
                message_ref[slot, piece] = total[start : start + 2, at]
            message_ref[slot, 4] = tags[0:2, at]


def scan_kernel(message_ref, out_ref):
    carried = [jnp.zeros((2, 128), F32) for _ in range(4)]
    for chip in range(CHIPS):
        tags = message_ref[chip, 4].astype(F32)
        factor = tags[0:1] + tags[1:2]
        for piece in range(4):
            high = carried[piece].astype(BF16)
            out_ref[chip, piece] = high
            out_ref[chip, piece + 4] = (carried[piece] - high.astype(F32)).astype(BF16)
            carried[piece] = factor * carried[piece] + message_ref[chip, piece].astype(F32)


def enter_kernel(came_ref, first_ref, keep_ref, send_ref):
    core = lax.axis_index("core")
    is_first = jnp.full((1, 1), core, jnp.int32) == 0
    for group in range(STATE // 8):
        for lane in range(HALF // 128):
            at = slice(lane * 128, (lane + 1) * 128)
            rows = slice(group * 8, group * 8 + 8)
            slot = group * (HALF // 128) + lane
            even = jnp.concatenate(
                [
                    came_ref[slot, piece].astype(F32) + came_ref[slot, piece + 4].astype(F32)
                    for piece in range(4)
                ],
                axis=0,
            )
            odd = first_ref[STATE : STATE + 1, at] * even + first_ref[rows, at]
            keep_ref[rows, at] = jnp.where(is_first, even, odd).astype(BF16)
            send_ref[rows, at] = jnp.where(is_first, odd, even).astype(BF16)


def within_kernel(
    early_ref, pm_ref, step_rows, log_rows, log_columns, now_ref, gate_ref, halo_ref, recv_ref,
    x_ref, proj_ref, tapx_ref, tapp_ref, within_ref, read_ref, outer_ref, xm_ref, write_ref,
    ext_ref, extp_ref,
):
    is_first = first_core()
    halo = halo_ref[...].astype(F32)
    came = jnp.concatenate(
        [
            recv_ref[STATE + 8 : STATE + 16],
            recv_ref[STATE + 16 : STATE + 24],
            recv_ref[STATE + 24 :, : 2 * STATE],
        ],
        axis=1,
    )
    halo = jnp.where(is_first, halo, came)
    xm, pm = first_of(
        halo[:, :CHANNELS], halo[:, CHANNELS:], x_ref[:8].astype(F32), proj_ref[:8].astype(F32),
        tapx_ref[...], tapp_ref[...], ext_ref, extp_ref,
    )
    token = lax.broadcasted_iota(jnp.int32, (8, 1), 0)

    def with_first(new, old):
        return jnp.where(token < 3, new.astype(F32), old.astype(F32)).astype(BF16)

    xm_ref[:8] = with_first(xm, early_ref[:8])
    xm_ref[8:] = early_ref[8:]
    pm = with_first(pm, pm_ref[:8])
    write_ref[:8] = pm[:, :STATE]
    write_ref[8:] = pm_ref[8:, :STATE]
    read_ref[:8] = pm[:, STATE:]
    read_ref[8:] = pm_ref[8:, STATE:]
    scores = dot(read_ref[...], write_ref[...], ((1,), (1,)))
    row = lax.broadcasted_iota(jnp.int32, (128, 128), 0)
    col = lax.broadcasted_iota(jnp.int32, (128, 128), 1)
    causal = col <= row
    left = lax.broadcasted_iota(jnp.int32, (128, 128), 1) < HEAD_DIM
    for pair in range(HEADS_LOCAL // 2):
        at = slice(pair * 128, (pair + 1) * 128)
        outs = []
        for head in (2 * pair, 2 * pair + 1):
            tops = []
            for t in range(2):
                parts = []
                trow = slice(t * 128, (t + 1) * 128)
                log_t = log_columns[trow, head : head + 1]
                for s in range(t + 1):
                    scol = slice(s * 128, (s + 1) * 128)
                    gap = log_t - log_rows[head : head + 1, scol]
                    if s == t:
                        gap = jnp.where(causal, gap, 0.0)
                    mix = scores[trow, scol] * jnp.exp2(gap) * step_rows[head : head + 1, scol]
                    if s == t:
                        mix = jnp.where(causal, mix, 0.0)
                    parts.append(mix.astype(BF16))
                mixing = parts[0] if t == 0 else jnp.concatenate(parts, axis=1)
                tops.append(dot(mixing, xm_ref[: (t + 1) * 128, at]))
            outs.append(tops)
        for t in range(2):
            trow = slice(t * 128, (t + 1) * 128)
            gates = silu(gate_ref[trow, at].astype(F32))
            outer_ref[trow, at] = now_ref[trow, at] * gates
            within_ref[trow, at] = jnp.where(left, outs[0][t], outs[1][t]) * gates


def gate_kernel(keep_ref, recv_ref, read_ref, within_ref, outer_ref, gated_ref, square_ref):
    core = lax.axis_index("core")
    is_first = jnp.full((1, 1), core, jnp.int32) == 0
    partial = jnp.zeros((TOKENS_LOCAL, 128), F32)
    for half in range(2):
        at = slice(half * HALF, (half + 1) * HALF)
        if half == 0:
            state = jnp.where(is_first, keep_ref[...], recv_ref[...])
        else:
            state = jnp.where(is_first, recv_ref[...], keep_ref[...])
        gated = within_ref[:, at] + outer_ref[:, at] * dot(read_ref[...], state)
        gated_ref[:, at] = gated
        square = gated * gated
        for lane in range(HALF // 128):
            partial = partial + square[:, lane * 128 : (lane + 1) * 128]
    total = jnp.sum(jnp.transpose(partial), axis=0, keepdims=True)
    row = lax.broadcasted_iota(jnp.int32, (8, 128), 0)
    block = jnp.where(row == 0, total[:, :128], jnp.where(row == 1, total[:, 128:], 0.0))
    for peer in range(4):
        square_ref[peer] = block


def norm_kernel(gated_ref, square_ref, gain_ref, out_ref, near_out_ref, sems):
    total = jnp.sum(square_ref[...], axis=0)
    scale = lax.rsqrt(total / (HEADS * HEAD_DIM) + 1.0)
    wide = jnp.concatenate(
        [jnp.broadcast_to(scale[0:1], (128, 128)), jnp.broadcast_to(scale[1:2], (128, 128))], axis=1
    )
    column = jnp.transpose(wide)
    chunks = 4
    size = TOKENS_LOCAL // chunks
    copies = []
    for chunk in range(chunks):
        rows = slice(chunk * size, (chunk + 1) * size)
        for lane in range(CHANNELS // 128):
            at = slice(lane * 128, (lane + 1) * 128)
            near_out_ref[rows, at] = (
                gated_ref[rows, at] * column[rows] * gain_ref[:, at]
            ).astype(BF16)
        here = pl.ds(chunk * size, size)
        copies.append(
            pltpu.make_async_copy(near_out_ref.at[here], out_ref.at[here], sems.at[chunk])
        )
        copies[-1].start()
    for copy in copies:
        copy.wait()


def shape(dims, dtype):
    return pltpu.VMEM(dims, dtype)


def call(kernel, outs, scratch=(), flops=0, **specs):
    cost = pl.CostEstimate(flops=flops, transcendentals=0, bytes_accessed=0) if flops else None
    return pl.pallas_call(
        kernel,
        out_shape=outs,
        scratch_shapes=scratch,
        cost_estimate=cost,
        compiler_params=pltpu.CompilerParams(vmem_limit_bytes=24 * 1024 * 1024),
        **specs,
    )


def near(value):
    return pltpu.with_memory_space_constraint(value, pltpu.VMEM)


def far(value):
    return pltpu.with_memory_space_constraint(value, pltpu.HBM)


ANY = pl.BlockSpec(memory_space=pl.ANY)
NEAR = pl.BlockSpec(memory_space=pltpu.VMEM)


def shards(
    seq_inputs, gate_inputs, projections, step_raw, step_bias, decay_rate, conv_feature, conv_proj,
    norm_gain,
):
    x = far(seq_inputs[0])
    proj = far(projections[0])
    step_rows = jnp.transpose(step_raw[0])
    chips = ("y", "z")
    rows = STATE + 32
    whole = (TOKENS_LOCAL, CHANNELS)
    prepared = (
        shape((HEADS_LOCAL, TOKENS_LOCAL), F32),
        shape((HEADS_LOCAL, TOKENS_LOCAL), F32),
        shape((TOKENS_LOCAL, 128), F32),
        shape((8, CHANNELS), F32),
        shape(whole, F32),
        shape(whole, BF16),
        shape((TOKENS_LOCAL, 2 * STATE), BF16),
        shape(whole, F32),
        shape((8, CHANNELS), F32),
        shape((4, CHANNELS), F32),
        shape((4, 2 * STATE), F32),
    )
    sources = (
        x, proj, far(step_rows), far(step_bias[None]), far(decay_rate[None]),
        far(conv_feature), far(conv_proj),
    )
    loads = [
        pltpu.VMEM((HEADS_LOCAL, TOKENS_LOCAL), F32),
        pltpu.VMEM((1, HEADS_LOCAL), F32),
        pltpu.VMEM((1, HEADS_LOCAL), F32),
        pltpu.SemaphoreType.DMA((9,)),
    ]
    tail, *early = call(
        early_kernel,
        (shape((8, CHANNELS + 2 * STATE), BF16),) + prepared,
        loads,
        in_specs=[ANY] * 7,
    )(*sources)
    halo = lax.ppermute(tail, ("y", "z", "core"), [(i, i + 1) for i in range(1, 2 * CHIPS - 1, 2)])
    (
        step, log_rows, log_columns, _, now, near_x, near_proj, _, end, tapx, tapp,
        xm, pm, sums, send,
    ) = call(
        state_kernel,
        prepared
        + (
            shape(whole, BF16),
            shape((TOKENS_LOCAL, 2 * STATE), BF16),
            shape((2, rows, HALF), F32),
            shape((rows, HALF), F32),
        ),
        loads,
        10**9,
        in_specs=[ANY] * 7 + [NEAR] * 11,
        input_output_aliases={7 + i: i for i in range(11)},
    )(*sources, *(near(value) for value in early))
    swap = [(0, 1), (1, 0)]
    other = lax.ppermute(send, "core", swap)
    small = [pltpu.VMEM((16, CHANNELS), F32), pltpu.VMEM((16, 2 * STATE), F32)]
    ranks = shape((8, HALF + STATE), BF16)
    own_rows, rows_send = call(first_kernel, (ranks, ranks), small)(
        near(halo), near(near_x), near(near_proj), near(end), near(tapx), near(tapp)
    )
    came_rows = lax.ppermute(rows_send, "core", [(0, 1)])
    message, first = call(
        join_kernel,
        (shape((CHIPS, 5, 2, 128), BF16), shape((STATE + 8, HALF), F32)),
        [pltpu.VMEM((16, HALF), F32), pltpu.VMEM((16, 2 * STATE), F32)],
    )(
        near(sums), near(other), near(near_x), near(near_proj), near(tapx), near(tapp),
        near(own_rows), near(came_rows),
    )
    gathered = lax.all_to_all(message, chips, 0, 0, tiled=True)
    entering = call(scan_kernel, shape((CHIPS, 8, 2, 128), BF16))(near(gathered))
    returned = lax.all_to_all(entering, chips, 0, 0, tiled=True)
    keep, give = call(
        enter_kernel, (shape((STATE, HALF), BF16), shape((STATE, HALF), BF16))
    )(near(returned), near(first))
    got = lax.ppermute(give, "core", swap)
    within, read, outer = call(
        within_kernel,
        (shape(whole, F32), shape((TOKENS_LOCAL, STATE), BF16), shape(whole, F32)),
        [pltpu.VMEM(whole, BF16), pltpu.VMEM((TOKENS_LOCAL, STATE), BF16)] + small,
        10**10,
    )(
        near(xm), near(pm), near(step), near(log_rows), near(log_columns), near(now),
        gate_inputs[0], near(halo), near(other), near(near_x), near(near_proj), near(tapx),
        near(tapp),
    )
    gated, square = call(
        gate_kernel, (shape((TOKENS_LOCAL, CHANNELS), F32), shape((4, 8, 128), F32))
    )(near(keep), near(got), near(read), near(within), near(outer))
    squares = lax.all_to_all(square, "head", 0, 0, tiled=True)
    out = call(
        norm_kernel,
        pltpu.HBM((TOKENS_LOCAL, CHANNELS), BF16),
        [pltpu.VMEM((TOKENS_LOCAL, CHANNELS), BF16), pltpu.SemaphoreType.DMA((4,))],
        out_specs=ANY,
    )(near(gated), near(squares), norm_gain[None])
    return out[None]


def solution(mesh):
    grid = Mesh(mesh.devices.reshape(8, 8, 2, 4), ("y", "z", "core", "head"))
    seq = ("y", "z", "core")
    return jax.shard_map(
        shards,
        mesh=grid,
        in_specs=(
            P(None, seq, "head"),
            P(None, seq, "head"),
            P(None, seq, None),
            P(None, seq, "head"),
            P("head"),
            P("head"),
            P(None, "head"),
            P(),
            P("head"),
        ),
        out_specs=P(None, seq, "head"),
        check_vma=False,
    )
```

```python
import jax
import jax.numpy as jnp
from jax import lax
from jax.experimental import pallas as pl
from jax.experimental.pallas import tpu as pltpu
from jax.sharding import Mesh, PartitionSpec as P

HEADS = 64
HEAD_DIM = 64
TOKENS_LOCAL = 256
CHANNELS = 1024
HALF = 512
STATE = 128
HEADS_LOCAL = 16
CHIPS = 64
LOG2E = 1.4426950408889634
F32 = jnp.float32
BF16 = jnp.bfloat16


def silu(value):
    half = 0.5 * value
    return half + half * jnp.tanh(half)


def parts_of(value):
    high = value.astype(BF16)
    rest = value - high.astype(F32)
    middle = rest.astype(BF16)
    low = (rest - middle.astype(F32)).astype(BF16)
    return high, middle, low


def dot(left, right, dims=((1,), (0,))):
    return lax.dot_general(left, right, (dims, ((), ())), preferred_element_type=F32)


def conv_silu(values, taps):
    values = values.astype(F32)
    running = values * taps[0:1]
    for k in range(1, 4):
        running = pltpu.roll(running, 1, 0) + values * taps[k : k + 1]
    return silu(running).astype(BF16)


def conv_first(ext_ref, taps, width):
    at = slice(0, width)
    running = ext_ref[5:13, at] * taps[0:1]
    for k in range(1, 4):
        running = running + ext_ref[5 + k : 13 + k, at] * taps[k : k + 1]
    return silu(running).astype(BF16)


def copy_all(pairs, sems):
    copies = [
        pltpu.make_async_copy(source, target, sems.at[place])
        for place, (source, target) in enumerate(pairs)
    ]
    for copy in copies:
        copy.start()
    return copies


def column_of(row):
    first = lax.broadcasted_iota(jnp.int32, (HEADS_LOCAL, HEADS_LOCAL), 0)
    second = lax.broadcasted_iota(jnp.int32, (HEADS_LOCAL, HEADS_LOCAL), 1)
    return jnp.sum(jnp.where(first == second, row, 0.0), axis=1, keepdims=True)


def prepare(
    x_ref, proj_ref, step_ref, bias_ref, rate_ref, tapx_ref, tapp_ref,
    step_out_ref, log_rows_ref, log_columns_ref, factor_ref, now_ref,
    near_x, near_proj, to_end_ref, end_ref, near_tapx, near_tapp,
    near_step, near_bias, near_rate, sems, tail_ref=None,
):
    pairs = [(step_ref, near_step), (bias_ref, near_bias), (rate_ref, near_rate)]
    if tail_ref is not None:
        rows = pl.ds(TOKENS_LOCAL - 8, 8)
        pairs += [
            (x_ref.at[rows], tail_ref.at[:, pl.ds(0, CHANNELS)]),
            (proj_ref.at[rows], tail_ref.at[:, pl.ds(CHANNELS, 2 * STATE)]),
        ]
    pairs += [
        (proj_ref, near_proj),
        (x_ref, near_x),
        (tapx_ref, near_tapx),
        (tapp_ref, near_tapp),
    ]
    copies = copy_all(pairs, sems)
    row = lax.broadcasted_iota(jnp.int32, (TOKENS_LOCAL, TOKENS_LOCAL), 0)
    col = lax.broadcasted_iota(jnp.int32, (TOKENS_LOCAL, TOKENS_LOCAL), 1)
    upper = (row <= col).astype(BF16)
    head = lax.broadcasted_iota(jnp.int32, (3 * HEADS_LOCAL, CHANNELS), 0)
    channel = lax.broadcasted_iota(jnp.int32, (3 * HEADS_LOCAL, CHANNELS), 1)
    spread = (channel // HEAD_DIM == head % HEADS_LOCAL).astype(BF16)

    def stacked(value):
        return jnp.concatenate(parts_of(value), axis=0)

    def to_channels(value):
        return dot(stacked(value), spread, ((0,), (0,)))

    for copy in copies[:3]:
        copy.wait()
    raw = near_step[...] + column_of(near_bias[...])
    step = jnp.maximum(raw, 0.0) + jnp.log1p(jnp.exp(-jnp.abs(raw)))
    sums = dot(stacked(step * -column_of(near_rate[...])), upper)
    log_decay = sums[:HEADS_LOCAL] + sums[HEADS_LOCAL : 2 * HEADS_LOCAL] + sums[2 * HEADS_LOCAL :]
    step_out_ref[...] = step
    log2 = log_decay * LOG2E
    log_rows_ref[...] = log2
    pad = jnp.zeros((128 - HEADS_LOCAL, TOKENS_LOCAL), F32)
    log_columns_ref[...] = jnp.transpose(jnp.concatenate([log2, pad], axis=0))
    last = log_decay[:, TOKENS_LOCAL - 1 :]
    to_end_ref[...] = to_channels(jnp.exp(last - log_decay) * step)
    factor_ref[...] = to_channels(jnp.broadcast_to(jnp.exp(last), (HEADS_LOCAL, 8)))
    now_ref[...] = to_channels(jnp.exp(log_decay))
    token = lax.broadcasted_iota(jnp.int32, (8, 1), 0)
    end_ref[...] = jnp.where(token < 3, to_end_ref[:8], 0.0)
    to_end_ref[:8] = jnp.where(token < 3, 0.0, to_end_ref[:8])
    for copy in copies[3:]:
        copy.wait()


def early_kernel(*refs):
    inputs, tail_ref, rest = refs[:7], refs[7], refs[8:]

    @pl.when(lax.axis_index("core") == 1)
    def _():
        prepare(*inputs, *rest, tail_ref=tail_ref)


def state_kernel(*refs):
    inputs, rest = refs[:7], refs[18:]
    outputs, (xm_ref, pm_ref, sums_ref), scratch = rest[:11], rest[11:14], rest[14:]
    factor_ref = outputs[3]
    near_x, near_proj, to_end_ref, end_ref, tapx_ref, tapp_ref = outputs[5:11]
    core = lax.axis_index("core")

    @pl.when(core == 0)
    def _():
        prepare(*inputs, *outputs, *scratch)

    is_first = first_core()
    pm = conv_silu(near_proj[...], tapp_ref[...])
    pm_ref[...] = pm
    turned = jnp.transpose(pm[:, :STATE].astype(F32)).astype(BF16)
    width = 256
    for tile in range(CHANNELS // width):
        at = slice(tile * width, (tile + 1) * width)
        xm = conv_silu(near_x[:, at], tapx_ref[:, at])
        xm_ref[:, at] = xm
        weighted = (xm.astype(F32) * to_end_ref[:, at]).astype(BF16)
        half, inside = divmod(tile * width, HALF)
        sums_ref[half, :STATE, inside : inside + width] = dot(turned, weighted)
    head_x = near_x[:8].astype(F32)
    head_proj = near_proj[:8].astype(F32)
    tail_x = near_x[-8:].astype(F32)
    tail_proj = near_proj[-8:].astype(F32)
    for half in range(2):
        at = slice(half * HALF, (half + 1) * HALF)
        sums_ref[half, STATE : STATE + 8] = factor_ref[:, at]
        sums_ref[half, STATE + 8 : STATE + 16] = jnp.where(
            is_first, tail_x[:, :HALF], head_x[:, at]
        )
        sums_ref[half, STATE + 16 : STATE + 24] = jnp.where(
            is_first, tail_x[:, HALF:], end_ref[:, at]
        )
        sums_ref[half, STATE + 24 :, : 2 * STATE] = jnp.where(is_first, tail_proj, head_proj)
        sums_ref[half, STATE + 24 :, 2 * STATE :] = jnp.zeros((8, HALF - 2 * STATE), F32)


def first_of(halo_x, halo_proj, head_x, head_proj, tapx, tapp, ext_ref, extp_ref):
    width = halo_x.shape[1]
    ext_ref[:8] = halo_x
    ext_ref[8:] = head_x
    extp_ref[:8] = halo_proj
    extp_ref[8:] = head_proj
    pm = conv_first(extp_ref, tapp, 2 * STATE)
    return conv_first(ext_ref, tapx, width), pm


def first_core():
    return jnp.full((1, 1), lax.axis_index("core"), jnp.int32) == 0


def first_kernel(
    halo_ref, x_ref, proj_ref, end_ref, tapx_ref, tapp_ref, before_ref, sums_ref, send_ref,
    ext_ref, extp_ref,
):
    core = lax.axis_index("core")
    halo = halo_ref[...].astype(F32)
    xm, pm = first_of(
        halo[:, :CHANNELS], halo[:, CHANNELS:], x_ref[:8].astype(F32), proj_ref[:8].astype(F32),
        tapx_ref[...], tapp_ref[...], ext_ref, extp_ref,
    )
    end = jnp.where(first_core(), end_ref[...], 0.0)
    added = dot(pm[:, :STATE], (xm.astype(F32) * end).astype(BF16), ((0,), (0,)))
    for half in range(2):
        at = slice(half * HALF, (half + 1) * HALF)
        sums_ref[half, :STATE] = before_ref[half, :STATE] + added[:, at]
    send_ref[...] = sums_ref[1 - core]


def join_kernel(
    sums_ref, recv_ref, x_ref, proj_ref, tapx_ref, tapp_ref, message_ref, first_ref, ext_ref,
    extp_ref,
):
    core = lax.axis_index("core")
    is_first = first_core()
    own = sums_ref[core]
    other = recv_ref[...]
    tail_x = x_ref[-8:].astype(F32)
    tail_proj = proj_ref[-8:].astype(F32)
    taps = tapx_ref[...]
    xm, pm = first_of(
        jnp.where(is_first, tail_x[:, :HALF], other[STATE + 16 : STATE + 24]),
        jnp.where(is_first, tail_proj, other[STATE + 24 :, : 2 * STATE]),
        jnp.where(is_first, other[STATE + 8 : STATE + 16], own[STATE + 8 : STATE + 16]),
        jnp.where(is_first, other[STATE + 24 :, : 2 * STATE], own[STATE + 24 :, : 2 * STATE]),
        jnp.where(is_first, taps[:, :HALF], taps[:, HALF:]),
        tapp_ref[...],
        ext_ref,
        extp_ref,
    )
    end = jnp.where(is_first, other[STATE + 16 : STATE + 24], own[STATE + 16 : STATE + 24])
    added = dot(pm[:, :STATE], (xm.astype(F32) * end).astype(BF16), ((0,), (0,)))
    first = jnp.where(is_first, own[: STATE + 8], other[: STATE + 8])
    second = jnp.where(is_first, other[: STATE + 8], own[: STATE + 8])
    first_ref[...] = first
    factor = second[STATE:] * first[STATE:]
    total = second[STATE : STATE + 1] * first[:STATE] + (second[:STATE] + added)
    high = factor.astype(BF16)
    low = (factor - high.astype(F32)).astype(BF16)
    row = lax.broadcasted_iota(jnp.int32, (8, HALF), 0)
    tags = jnp.where(row == 0, high.astype(F32), low.astype(F32)).astype(BF16)
    total = total.astype(BF16)
    for group in range(STATE // 8):
        for lane in range(HALF // 128):
            at = slice(lane * 128, (lane + 1) * 128)
            slot = group * (HALF // 128) + lane
            for piece in range(4):
                start = group * 8 + piece * 2
                message_ref[slot, piece] = total[start : start + 2, at]
            message_ref[slot, 4] = tags[0:2, at]


def scan_kernel(message_ref, out_ref):
    carried = [jnp.zeros((2, 128), F32) for _ in range(4)]
    for chip in range(CHIPS):
        tags = message_ref[chip, 4].astype(F32)
        factor = tags[0:1] + tags[1:2]
        for piece in range(4):
            high = carried[piece].astype(BF16)
            out_ref[chip, piece] = high
            out_ref[chip, piece + 4] = (carried[piece] - high.astype(F32)).astype(BF16)
            carried[piece] = factor * carried[piece] + message_ref[chip, piece].astype(F32)


def enter_kernel(came_ref, first_ref, keep_ref, send_ref):
    core = lax.axis_index("core")
    is_first = jnp.full((1, 1), core, jnp.int32) == 0
    for group in range(STATE // 8):
        for lane in range(HALF // 128):
            at = slice(lane * 128, (lane + 1) * 128)
            rows = slice(group * 8, group * 8 + 8)
            slot = group * (HALF // 128) + lane
            even = jnp.concatenate(
                [
                    came_ref[slot, piece].astype(F32) + came_ref[slot, piece + 4].astype(F32)
                    for piece in range(4)
                ],
                axis=0,
            )
            odd = first_ref[STATE : STATE + 1, at] * even + first_ref[rows, at]
            keep_ref[rows, at] = jnp.where(is_first, even, odd).astype(BF16)
            send_ref[rows, at] = jnp.where(is_first, odd, even).astype(BF16)


def within_kernel(
    early_ref, pm_ref, step_rows, log_rows, log_columns, now_ref, gate_ref, halo_ref, recv_ref,
    x_ref, proj_ref, tapx_ref, tapp_ref, within_ref, read_ref, outer_ref, xm_ref, write_ref,
    ext_ref, extp_ref,
):
    is_first = first_core()
    halo = halo_ref[...].astype(F32)
    came = jnp.concatenate(
        [
            recv_ref[STATE + 8 : STATE + 16],
            recv_ref[STATE + 16 : STATE + 24],
            recv_ref[STATE + 24 :, : 2 * STATE],
        ],
        axis=1,
    )
    halo = jnp.where(is_first, halo, came)
    xm, pm = first_of(
        halo[:, :CHANNELS], halo[:, CHANNELS:], x_ref[:8].astype(F32), proj_ref[:8].astype(F32),
        tapx_ref[...], tapp_ref[...], ext_ref, extp_ref,
    )
    token = lax.broadcasted_iota(jnp.int32, (8, 1), 0)

    def with_first(new, old):
        return jnp.where(token < 3, new.astype(F32), old.astype(F32)).astype(BF16)

    xm_ref[:8] = with_first(xm, early_ref[:8])
    xm_ref[8:] = early_ref[8:]
    pm = with_first(pm, pm_ref[:8])
    write_ref[:8] = pm[:, :STATE]
    write_ref[8:] = pm_ref[8:, :STATE]
    read_ref[:8] = pm[:, STATE:]
    read_ref[8:] = pm_ref[8:, STATE:]
    scores = dot(read_ref[...], write_ref[...], ((1,), (1,)))
    row = lax.broadcasted_iota(jnp.int32, (128, 128), 0)
    col = lax.broadcasted_iota(jnp.int32, (128, 128), 1)
    causal = col <= row
    left = lax.broadcasted_iota(jnp.int32, (128, 128), 1) < HEAD_DIM
    for pair in range(HEADS_LOCAL // 2):
        at = slice(pair * 128, (pair + 1) * 128)
        outs = []
        for head in (2 * pair, 2 * pair + 1):
            tops = []
            for t in range(2):
                parts = []
                trow = slice(t * 128, (t + 1) * 128)
                log_t = log_columns[trow, head : head + 1]
                for s in range(t + 1):
                    scol = slice(s * 128, (s + 1) * 128)
                    gap = log_t - log_rows[head : head + 1, scol]
                    if s == t:
                        gap = jnp.where(causal, gap, 0.0)
                    mix = scores[trow, scol] * jnp.exp2(gap) * step_rows[head : head + 1, scol]
                    if s == t:
                        mix = jnp.where(causal, mix, 0.0)
                    parts.append(mix.astype(BF16))
                mixing = parts[0] if t == 0 else jnp.concatenate(parts, axis=1)
                tops.append(dot(mixing, xm_ref[: (t + 1) * 128, at]))
            outs.append(tops)
        for t in range(2):
            trow = slice(t * 128, (t + 1) * 128)
            gates = silu(gate_ref[trow, at].astype(F32))
            outer_ref[trow, at] = now_ref[trow, at] * gates
            within_ref[trow, at] = jnp.where(left, outs[0][t], outs[1][t]) * gates


def gate_kernel(keep_ref, recv_ref, read_ref, within_ref, outer_ref, gated_ref, square_ref):
    core = lax.axis_index("core")
    is_first = jnp.full((1, 1), core, jnp.int32) == 0
    partial = jnp.zeros((TOKENS_LOCAL, 128), F32)
    for half in range(2):
        at = slice(half * HALF, (half + 1) * HALF)
        if half == 0:
            state = jnp.where(is_first, keep_ref[...], recv_ref[...])
        else:
            state = jnp.where(is_first, recv_ref[...], keep_ref[...])
        gated = within_ref[:, at] + outer_ref[:, at] * dot(read_ref[...], state)
        gated_ref[:, at] = gated
        square = gated * gated
        for lane in range(HALF // 128):
            partial = partial + square[:, lane * 128 : (lane + 1) * 128]
    total = jnp.sum(jnp.transpose(partial), axis=0, keepdims=True)
    row = lax.broadcasted_iota(jnp.int32, (8, 128), 0)
    block = jnp.where(row == 0, total[:, :128], jnp.where(row == 1, total[:, 128:], 0.0))
    for peer in range(4):
        square_ref[peer] = block


def norm_kernel(gated_ref, square_ref, gain_ref, out_ref, near_out_ref, sems):
    total = jnp.sum(square_ref[...], axis=0)
    scale = lax.rsqrt(total / (HEADS * HEAD_DIM) + 1.0)
    wide = jnp.concatenate(
        [jnp.broadcast_to(scale[0:1], (128, 128)), jnp.broadcast_to(scale[1:2], (128, 128))], axis=1
    )
    column = jnp.transpose(wide)
    chunks = 4
    size = TOKENS_LOCAL // chunks
    copies = []
    for chunk in range(chunks):
        rows = slice(chunk * size, (chunk + 1) * size)
        for lane in range(CHANNELS // 128):
            at = slice(lane * 128, (lane + 1) * 128)
            near_out_ref[rows, at] = (
                gated_ref[rows, at] * column[rows] * gain_ref[:, at]
            ).astype(BF16)
        here = pl.ds(chunk * size, size)
        copies.append(
            pltpu.make_async_copy(near_out_ref.at[here], out_ref.at[here], sems.at[chunk])
        )
        copies[-1].start()
    for copy in copies:
        copy.wait()


def shape(dims, dtype):
    return pltpu.VMEM(dims, dtype)


def call(kernel, outs, scratch=(), flops=0, **specs):
    cost = pl.CostEstimate(flops=flops, transcendentals=0, bytes_accessed=0) if flops else None
    return pl.pallas_call(
        kernel,
        out_shape=outs,
        scratch_shapes=scratch,
        cost_estimate=cost,
        compiler_params=pltpu.CompilerParams(vmem_limit_bytes=24 * 1024 * 1024),
        **specs,
    )


def near(value):
    return pltpu.with_memory_space_constraint(value, pltpu.VMEM)


def far(value):
    return pltpu.with_memory_space_constraint(value, pltpu.HBM)


ANY = pl.BlockSpec(memory_space=pl.ANY)
NEAR = pl.BlockSpec(memory_space=pltpu.VMEM)


def shards(
    seq_inputs, gate_inputs, projections, step_raw, step_bias, decay_rate, conv_feature, conv_proj,
    norm_gain,
):
    x = far(seq_inputs[0])
    proj = far(projections[0])
    step_rows = jnp.transpose(step_raw[0])
    chips = ("y", "z")
    rows = STATE + 32
    whole = (TOKENS_LOCAL, CHANNELS)
    prepared = (
        shape((HEADS_LOCAL, TOKENS_LOCAL), F32),
        shape((HEADS_LOCAL, TOKENS_LOCAL), F32),
        shape((TOKENS_LOCAL, 128), F32),
        shape((8, CHANNELS), F32),
        shape(whole, F32),
        shape(whole, BF16),
        shape((TOKENS_LOCAL, 2 * STATE), BF16),
        shape(whole, F32),
        shape((8, CHANNELS), F32),
        shape((4, CHANNELS), F32),
        shape((4, 2 * STATE), F32),
    )
    sources = (
        x, proj, far(step_rows), far(step_bias[None]), far(decay_rate[None]),
        far(conv_feature), far(conv_proj),
    )
    loads = [
        pltpu.VMEM((HEADS_LOCAL, TOKENS_LOCAL), F32),
        pltpu.VMEM((1, HEADS_LOCAL), F32),
        pltpu.VMEM((1, HEADS_LOCAL), F32),
        pltpu.SemaphoreType.DMA((9,)),
    ]
    tail, *early = call(
        early_kernel,
        (shape((8, CHANNELS + 2 * STATE), BF16),) + prepared,
        loads,
        in_specs=[ANY] * 7,
    )(*sources)
    halo = lax.ppermute(tail, ("y", "z", "core"), [(i, i + 1) for i in range(1, 2 * CHIPS - 1, 2)])
    (
        step, log_rows, log_columns, _, now, near_x, near_proj, _, end, tapx, tapp,
        xm, pm, before,
    ) = call(
        state_kernel,
        prepared
        + (
            shape(whole, BF16),
            shape((TOKENS_LOCAL, 2 * STATE), BF16),
            shape((2, rows, HALF), F32),
        ),
        loads,
        10**9,
        in_specs=[ANY] * 7 + [NEAR] * 11,
        input_output_aliases={7 + i: i for i in range(11)},
    )(*sources, *(near(value) for value in early))
    small = [pltpu.VMEM((16, CHANNELS), F32), pltpu.VMEM((16, 2 * STATE), F32)]
    sums, send = call(
        first_kernel,
        (shape((2, rows, HALF), F32), shape((rows, HALF), F32)),
        small,
        input_output_aliases={6: 0},
    )(
        near(halo), near(near_x), near(near_proj), near(end), near(tapx), near(tapp), near(before)
    )
    swap = [(0, 1), (1, 0)]
    other = lax.ppermute(send, "core", swap)
    message, first = call(
        join_kernel,
        (shape((CHIPS, 5, 2, 128), BF16), shape((STATE + 8, HALF), F32)),
        [pltpu.VMEM((16, HALF), F32), pltpu.VMEM((16, 2 * STATE), F32)],
    )(
        near(sums), near(other), near(near_x), near(near_proj), near(tapx), near(tapp),
    )
    gathered = lax.all_to_all(message, chips, 0, 0, tiled=True)
    entering = call(scan_kernel, shape((CHIPS, 8, 2, 128), BF16))(near(gathered))
    returned = lax.all_to_all(entering, chips, 0, 0, tiled=True)
    keep, give = call(
        enter_kernel, (shape((STATE, HALF), BF16), shape((STATE, HALF), BF16))
    )(near(returned), near(first))
    got = lax.ppermute(give, "core", swap)
    within, read, outer = call(
        within_kernel,
        (shape(whole, F32), shape((TOKENS_LOCAL, STATE), BF16), shape(whole, F32)),
        [pltpu.VMEM(whole, BF16), pltpu.VMEM((TOKENS_LOCAL, STATE), BF16)] + small,
        10**10,
    )(
        near(xm), near(pm), near(step), near(log_rows), near(log_columns), near(now),
        gate_inputs[0], near(halo), near(other), near(near_x), near(near_proj), near(tapx),
        near(tapp),
    )
    gated, square = call(
        gate_kernel, (shape((TOKENS_LOCAL, CHANNELS), F32), shape((4, 8, 128), F32))
    )(near(keep), near(got), near(read), near(within), near(outer))
    squares = lax.all_to_all(square, "head", 0, 0, tiled=True)
    out = call(
        norm_kernel,
        pltpu.HBM((TOKENS_LOCAL, CHANNELS), BF16),
        [pltpu.VMEM((TOKENS_LOCAL, CHANNELS), BF16), pltpu.SemaphoreType.DMA((4,))],
        out_specs=ANY,
    )(near(gated), near(squares), norm_gain[None])
    return out[None]


def solution(mesh):
    grid = Mesh(mesh.devices.reshape(8, 8, 2, 4), ("y", "z", "core", "head"))
    seq = ("y", "z", "core")
    return jax.shard_map(
        shards,
        mesh=grid,
        in_specs=(
            P(None, seq, "head"),
            P(None, seq, "head"),
            P(None, seq, None),
            P(None, seq, "head"),
            P("head"),
            P("head"),
            P(None, "head"),
            P(),
            P("head"),
        ),
        out_specs=P(None, seq, "head"),
        check_vma=False,
    )
```

```python
import jax
import jax.numpy as jnp
from jax import lax
from jax.experimental import pallas as pl
from jax.experimental.pallas import tpu as pltpu
from jax.sharding import Mesh, PartitionSpec as P

HEADS = 64
HEAD_DIM = 64
TOKENS_LOCAL = 256
CHANNELS = 1024
HALF = 512
STATE = 128
HEADS_LOCAL = 16
CHIPS = 64
LOG2E = 1.4426950408889634
F32 = jnp.float32
BF16 = jnp.bfloat16


def silu(value):
    half = 0.5 * value
    return half + half * jnp.tanh(half)


def parts_of(value):
    high = value.astype(BF16)
    rest = value - high.astype(F32)
    middle = rest.astype(BF16)
    low = (rest - middle.astype(F32)).astype(BF16)
    return high, middle, low


def dot(left, right, dims=((1,), (0,))):
    return lax.dot_general(left, right, (dims, ((), ())), preferred_element_type=F32)


def conv_silu(values, taps):
    values = values.astype(F32)
    running = values * taps[0:1]
    for k in range(1, 4):
        running = pltpu.roll(running, 1, 0) + values * taps[k : k + 1]
    return silu(running).astype(BF16)


def conv_first(ext_ref, taps, width):
    at = slice(0, width)
    running = ext_ref[5:13, at] * taps[0:1]
    for k in range(1, 4):
        running = running + ext_ref[5 + k : 13 + k, at] * taps[k : k + 1]
    return silu(running).astype(BF16)


def copy_all(pairs, sems):
    copies = [
        pltpu.make_async_copy(source, target, sems.at[place])
        for place, (source, target) in enumerate(pairs)
    ]
    for copy in copies:
        copy.start()
    return copies


def column_of(row):
    first = lax.broadcasted_iota(jnp.int32, (HEADS_LOCAL, HEADS_LOCAL), 0)
    second = lax.broadcasted_iota(jnp.int32, (HEADS_LOCAL, HEADS_LOCAL), 1)
    return jnp.sum(jnp.where(first == second, row, 0.0), axis=1, keepdims=True)


def prepare(
    x_ref, proj_ref, step_ref, bias_ref, rate_ref, tapx_ref, tapp_ref,
    step_out_ref, log_rows_ref, log_columns_ref, factor_ref, now_ref,
    near_x, near_proj, to_end_ref, end_ref, near_tapx, near_tapp,
    near_step, near_bias, near_rate, sems, tail_ref=None,
):
    pairs = [(step_ref, near_step), (bias_ref, near_bias), (rate_ref, near_rate)]
    if tail_ref is not None:
        rows = pl.ds(TOKENS_LOCAL - 8, 8)
        pairs += [
            (x_ref.at[rows], tail_ref.at[:, pl.ds(0, CHANNELS)]),
            (proj_ref.at[rows], tail_ref.at[:, pl.ds(CHANNELS, 2 * STATE)]),
        ]
    pairs += [
        (proj_ref, near_proj),
        (x_ref, near_x),
        (tapx_ref, near_tapx),
        (tapp_ref, near_tapp),
    ]
    copies = copy_all(pairs, sems)
    row = lax.broadcasted_iota(jnp.int32, (TOKENS_LOCAL, TOKENS_LOCAL), 0)
    col = lax.broadcasted_iota(jnp.int32, (TOKENS_LOCAL, TOKENS_LOCAL), 1)
    upper = (row <= col).astype(BF16)
    head = lax.broadcasted_iota(jnp.int32, (3 * HEADS_LOCAL, CHANNELS), 0)
    channel = lax.broadcasted_iota(jnp.int32, (3 * HEADS_LOCAL, CHANNELS), 1)
    spread = (channel // HEAD_DIM == head % HEADS_LOCAL).astype(BF16)

    def stacked(value):
        return jnp.concatenate(parts_of(value), axis=0)

    def to_channels(value):
        return dot(stacked(value), spread, ((0,), (0,)))

    for copy in copies[:3]:
        copy.wait()
    raw = near_step[...] + column_of(near_bias[...])
    step = jnp.maximum(raw, 0.0) + jnp.log1p(jnp.exp(-jnp.abs(raw)))
    sums = dot(stacked(step * -column_of(near_rate[...])), upper)
    log_decay = sums[:HEADS_LOCAL] + sums[HEADS_LOCAL : 2 * HEADS_LOCAL] + sums[2 * HEADS_LOCAL :]
    step_out_ref[...] = step
    log2 = log_decay * LOG2E
    log_rows_ref[...] = log2
    pad = jnp.zeros((128 - HEADS_LOCAL, TOKENS_LOCAL), F32)
    log_columns_ref[...] = jnp.transpose(jnp.concatenate([log2, pad], axis=0))
    last = log_decay[:, TOKENS_LOCAL - 1 :]
    to_end_ref[...] = to_channels(jnp.exp(last - log_decay) * step)
    factor_ref[...] = to_channels(jnp.broadcast_to(jnp.exp(last), (HEADS_LOCAL, 8)))
    now_ref[...] = to_channels(jnp.exp(log_decay))
    token = lax.broadcasted_iota(jnp.int32, (8, 1), 0)
    end_ref[...] = jnp.where(token < 3, to_end_ref[:8], 0.0)
    to_end_ref[:8] = jnp.where(token < 3, 0.0, to_end_ref[:8])
    for copy in copies[3:]:
        copy.wait()


def early_kernel(*refs):
    inputs, tail_ref, rest = refs[:7], refs[7], refs[8:]

    @pl.when(lax.axis_index("core") == 1)
    def _():
        prepare(*inputs, *rest, tail_ref=tail_ref)


def state_kernel(*refs):
    inputs, rest = refs[:7], refs[18:]
    outputs, (xm_ref, pm_ref, sums_ref, send_ref), scratch = rest[:11], rest[11:15], rest[15:]
    factor_ref = outputs[3]
    near_x, near_proj, to_end_ref, end_ref, tapx_ref, tapp_ref = outputs[5:11]
    core = lax.axis_index("core")

    @pl.when(core == 0)
    def _():
        prepare(*inputs, *outputs, *scratch)

    is_first = first_core()
    pm = conv_silu(near_proj[...], tapp_ref[...])
    pm_ref[...] = pm
    turned = jnp.transpose(pm[:, :STATE].astype(F32)).astype(BF16)
    width = 256
    for tile in range(CHANNELS // width):
        at = slice(tile * width, (tile + 1) * width)
        xm = conv_silu(near_x[:, at], tapx_ref[:, at])
        xm_ref[:, at] = xm
        weighted = (xm.astype(F32) * to_end_ref[:, at]).astype(BF16)
        half, inside = divmod(tile * width, HALF)
        sums_ref[half, :STATE, inside : inside + width] = dot(turned, weighted)
    head_x = near_x[:8].astype(F32)
    head_proj = near_proj[:8].astype(F32)
    tail_x = near_x[-8:].astype(F32)
    tail_proj = near_proj[-8:].astype(F32)
    for half in range(2):
        at = slice(half * HALF, (half + 1) * HALF)
        sums_ref[half, STATE : STATE + 8] = factor_ref[:, at]
        sums_ref[half, STATE + 8 : STATE + 16] = jnp.where(
            is_first, tail_x[:, :HALF], head_x[:, at]
        )
        sums_ref[half, STATE + 16 : STATE + 24] = jnp.where(
            is_first, tail_x[:, HALF:], end_ref[:, at]
        )
        sums_ref[half, STATE + 24 :, : 2 * STATE] = jnp.where(is_first, tail_proj, head_proj)
        sums_ref[half, STATE + 24 :, 2 * STATE :] = jnp.zeros((8, HALF - 2 * STATE), F32)
    send_ref[...] = sums_ref[1 - core]


def first_of(halo_x, halo_proj, head_x, head_proj, tapx, tapp, ext_ref, extp_ref):
    width = halo_x.shape[1]
    ext_ref[:8] = halo_x
    ext_ref[8:] = head_x
    extp_ref[:8] = halo_proj
    extp_ref[8:] = head_proj
    pm = conv_first(extp_ref, tapp, 2 * STATE)
    return conv_first(ext_ref, tapx, width), pm


def first_core():
    return jnp.full((1, 1), lax.axis_index("core"), jnp.int32) == 0


def first_kernel(
    halo_ref, x_ref, proj_ref, end_ref, tapx_ref, tapp_ref, own_ref, send_ref, ext_ref, extp_ref
):
    halo = halo_ref[...].astype(F32)
    xm, pm = first_of(
        halo[:, :CHANNELS], halo[:, CHANNELS:], x_ref[:8].astype(F32), proj_ref[:8].astype(F32),
        tapx_ref[...], tapp_ref[...], ext_ref, extp_ref,
    )
    weighted = (xm.astype(F32) * end_ref[...]).astype(BF16)
    own_ref[:, :HALF] = weighted[:, :HALF]
    own_ref[:, HALF:] = pm[:, :STATE]
    send_ref[:, :HALF] = weighted[:, HALF:]
    send_ref[:, HALF:] = pm[:, :STATE]


def join_kernel(
    sums_ref, recv_ref, x_ref, proj_ref, tapx_ref, tapp_ref, own_rows_ref, recv_rows_ref,
    message_ref, first_ref, ext_ref, extp_ref,
):
    core = lax.axis_index("core")
    is_first = first_core()
    own = sums_ref[core]
    other = recv_ref[...]
    tail_x = x_ref[-8:].astype(F32)
    tail_proj = proj_ref[-8:].astype(F32)
    taps = tapx_ref[...]
    xm, pm = first_of(
        jnp.where(is_first, tail_x[:, :HALF], other[STATE + 16 : STATE + 24]),
        jnp.where(is_first, tail_proj, other[STATE + 24 :, : 2 * STATE]),
        jnp.where(is_first, other[STATE + 8 : STATE + 16], own[STATE + 8 : STATE + 16]),
        jnp.where(is_first, other[STATE + 24 :, : 2 * STATE], own[STATE + 24 :, : 2 * STATE]),
        jnp.where(is_first, taps[:, :HALF], taps[:, HALF:]),
        tapp_ref[...],
        ext_ref,
        extp_ref,
    )
    end = jnp.where(is_first, other[STATE + 16 : STATE + 24], own[STATE + 16 : STATE + 24])
    added = dot(pm[:, :STATE], (xm.astype(F32) * end).astype(BF16), ((0,), (0,)))
    rows = jnp.where(
        is_first, own_rows_ref[...].astype(F32), recv_rows_ref[...].astype(F32)
    ).astype(BF16)
    added_first = dot(rows[:, HALF:], rows[:, :HALF], ((0,), (0,)))
    first = jnp.where(is_first, own[: STATE + 8], other[: STATE + 8])
    second = jnp.where(is_first, other[: STATE + 8], own[: STATE + 8])
    first_state = first[:STATE] + added_first
    first_ref[:STATE] = first_state
    first_ref[STATE:] = first[STATE:]
    factor = second[STATE:] * first[STATE:]
    total = second[STATE : STATE + 1] * first_state + (second[:STATE] + added)
    high = factor.astype(BF16)
    low = (factor - high.astype(F32)).astype(BF16)
    row = lax.broadcasted_iota(jnp.int32, (8, HALF), 0)
    tags = jnp.where(row == 0, high.astype(F32), low.astype(F32)).astype(BF16)
    total = total.astype(BF16)
    for group in range(STATE // 8):
        for lane in range(HALF // 128):
            at = slice(lane * 128, (lane + 1) * 128)
            slot = group * (HALF // 128) + lane
            for piece in range(4):
                start = group * 8 + piece * 2
                message_ref[slot, piece] = total[start : start + 2, at]
            message_ref[slot, 4] = tags[0:2, at]


def scan_kernel(message_ref, out_ref):
    carried = [jnp.zeros((2, 128), F32) for _ in range(4)]
    for chip in range(CHIPS):
        tags = message_ref[chip, 4].astype(F32)
        factor = tags[0:1] + tags[1:2]
        for piece in range(4):
            high = carried[piece].astype(BF16)
            out_ref[chip, piece] = high
            out_ref[chip, piece + 4] = (carried[piece] - high.astype(F32)).astype(BF16)
            carried[piece] = factor * carried[piece] + message_ref[chip, piece].astype(F32)


def enter_kernel(came_ref, first_ref, keep_ref, send_ref):
    core = lax.axis_index("core")
    is_first = jnp.full((1, 1), core, jnp.int32) == 0
    for group in range(STATE // 8):
        for lane in range(HALF // 128):
            at = slice(lane * 128, (lane + 1) * 128)
            rows = slice(group * 8, group * 8 + 8)
            slot = group * (HALF // 128) + lane
            even = jnp.concatenate(
                [
                    came_ref[slot, piece].astype(F32) + came_ref[slot, piece + 4].astype(F32)
                    for piece in range(4)
                ],
                axis=0,
            )
            odd = first_ref[STATE : STATE + 1, at] * even + first_ref[rows, at]
            keep_ref[rows, at] = jnp.where(is_first, even, odd).astype(BF16)
            send_ref[rows, at] = jnp.where(is_first, odd, even).astype(BF16)


def within_kernel(
    early_ref, pm_ref, step_rows, log_rows, log_columns, now_ref, gate_ref, halo_ref, recv_ref,
    x_ref, proj_ref, tapx_ref, tapp_ref, within_ref, read_ref, outer_ref, xm_ref, write_ref,
    ext_ref, extp_ref,
):
    is_first = first_core()
    halo = halo_ref[...].astype(F32)
    came = jnp.concatenate(
        [
            recv_ref[STATE + 8 : STATE + 16],
            recv_ref[STATE + 16 : STATE + 24],
            recv_ref[STATE + 24 :, : 2 * STATE],
        ],
        axis=1,
    )
    halo = jnp.where(is_first, halo, came)
    xm, pm = first_of(
        halo[:, :CHANNELS], halo[:, CHANNELS:], x_ref[:8].astype(F32), proj_ref[:8].astype(F32),
        tapx_ref[...], tapp_ref[...], ext_ref, extp_ref,
    )
    token = lax.broadcasted_iota(jnp.int32, (8, 1), 0)

    def with_first(new, old):
        return jnp.where(token < 3, new.astype(F32), old.astype(F32)).astype(BF16)

    xm_ref[:8] = with_first(xm, early_ref[:8])
    xm_ref[8:] = early_ref[8:]
    pm = with_first(pm, pm_ref[:8])
    write_ref[:8] = pm[:, :STATE]
    write_ref[8:] = pm_ref[8:, :STATE]
    read_ref[:8] = pm[:, STATE:]
    read_ref[8:] = pm_ref[8:, STATE:]
    scores = dot(read_ref[...], write_ref[...], ((1,), (1,)))
    row = lax.broadcasted_iota(jnp.int32, (128, 128), 0)
    col = lax.broadcasted_iota(jnp.int32, (128, 128), 1)
    causal = col <= row
    left = lax.broadcasted_iota(jnp.int32, (128, 128), 1) < HEAD_DIM
    for pair in range(HEADS_LOCAL // 2):
        at = slice(pair * 128, (pair + 1) * 128)
        outs = []
        for head in (2 * pair, 2 * pair + 1):
            tops = []
            for t in range(2):
                parts = []
                trow = slice(t * 128, (t + 1) * 128)
                log_t = log_columns[trow, head : head + 1]
                for s in range(t + 1):
                    scol = slice(s * 128, (s + 1) * 128)
                    gap = log_t - log_rows[head : head + 1, scol]
                    if s == t:
                        gap = jnp.where(causal, gap, 0.0)
                    mix = scores[trow, scol] * jnp.exp2(gap) * step_rows[head : head + 1, scol]
                    if s == t:
                        mix = jnp.where(causal, mix, 0.0)
                    parts.append(mix.astype(BF16))
                mixing = parts[0] if t == 0 else jnp.concatenate(parts, axis=1)
                tops.append(dot(mixing, xm_ref[: (t + 1) * 128, at]))
            outs.append(tops)
        for t in range(2):
            trow = slice(t * 128, (t + 1) * 128)
            gates = silu(gate_ref[trow, at].astype(F32))
            outer_ref[trow, at] = now_ref[trow, at] * gates
            within_ref[trow, at] = jnp.where(left, outs[0][t], outs[1][t]) * gates


def gate_kernel(keep_ref, recv_ref, read_ref, within_ref, outer_ref, gated_ref, square_ref):
    core = lax.axis_index("core")
    is_first = jnp.full((1, 1), core, jnp.int32) == 0
    partial = jnp.zeros((TOKENS_LOCAL, 128), F32)
    for half in range(2):
        at = slice(half * HALF, (half + 1) * HALF)
        if half == 0:
            state = jnp.where(is_first, keep_ref[...], recv_ref[...])
        else:
            state = jnp.where(is_first, recv_ref[...], keep_ref[...])
        gated = within_ref[:, at] + outer_ref[:, at] * dot(read_ref[...], state)
        gated_ref[:, at] = gated
        square = gated * gated
        for lane in range(HALF // 128):
            partial = partial + square[:, lane * 128 : (lane + 1) * 128]
    total = jnp.sum(jnp.transpose(partial), axis=0, keepdims=True)
    square_ref[0:1, :] = total[:, :128]
    square_ref[1:2, :] = total[:, 128:]


def norm_kernel(gated_ref, square_ref, gain_ref, out_ref, near_out_ref, sems):
    total = jnp.sum(square_ref[...], axis=0)
    scale = lax.rsqrt(total / (HEADS * HEAD_DIM) + 1.0)
    wide = jnp.concatenate(
        [jnp.broadcast_to(scale[0:1], (128, 128)), jnp.broadcast_to(scale[1:2], (128, 128))], axis=1
    )
    column = jnp.transpose(wide)
    chunks = 8
    size = TOKENS_LOCAL // chunks
    copies = []
    for chunk in range(chunks):
        rows = slice(chunk * size, (chunk + 1) * size)
        for lane in range(CHANNELS // 128):
            at = slice(lane * 128, (lane + 1) * 128)
            near_out_ref[rows, at] = (
                gated_ref[rows, at] * column[rows] * gain_ref[:, at]
            ).astype(BF16)
        here = pl.ds(chunk * size, size)
        copies.append(
            pltpu.make_async_copy(near_out_ref.at[here], out_ref.at[here], sems.at[chunk])
        )
        copies[-1].start()
    for copy in copies:
        copy.wait()


def shape(dims, dtype):
    return pltpu.VMEM(dims, dtype)


def call(kernel, outs, scratch=(), flops=0, **specs):
    cost = pl.CostEstimate(flops=flops, transcendentals=0, bytes_accessed=0) if flops else None
    return pl.pallas_call(
        kernel,
        out_shape=outs,
        scratch_shapes=scratch,
        cost_estimate=cost,
        compiler_params=pltpu.CompilerParams(vmem_limit_bytes=24 * 1024 * 1024),
        **specs,
    )


def near(value):
    return pltpu.with_memory_space_constraint(value, pltpu.VMEM)


def far(value):
    return pltpu.with_memory_space_constraint(value, pltpu.HBM)


ANY = pl.BlockSpec(memory_space=pl.ANY)
NEAR = pl.BlockSpec(memory_space=pltpu.VMEM)


def shards(
    seq_inputs, gate_inputs, projections, step_raw, step_bias, decay_rate, conv_feature, conv_proj,
    norm_gain,
):
    x = far(seq_inputs[0])
    proj = far(projections[0])
    step_rows = jnp.transpose(step_raw[0])
    chips = ("y", "z")
    rows = STATE + 32
    whole = (TOKENS_LOCAL, CHANNELS)
    prepared = (
        shape((HEADS_LOCAL, TOKENS_LOCAL), F32),
        shape((HEADS_LOCAL, TOKENS_LOCAL), F32),
        shape((TOKENS_LOCAL, 128), F32),
        shape((8, CHANNELS), F32),
        shape(whole, F32),
        shape(whole, BF16),
        shape((TOKENS_LOCAL, 2 * STATE), BF16),
        shape(whole, F32),
        shape((8, CHANNELS), F32),
        shape((4, CHANNELS), F32),
        shape((4, 2 * STATE), F32),
    )
    sources = (
        x, proj, far(step_rows), far(step_bias[None]), far(decay_rate[None]),
        far(conv_feature), far(conv_proj),
    )
    loads = [
        pltpu.VMEM((HEADS_LOCAL, TOKENS_LOCAL), F32),
        pltpu.VMEM((1, HEADS_LOCAL), F32),
        pltpu.VMEM((1, HEADS_LOCAL), F32),
        pltpu.SemaphoreType.DMA((9,)),
    ]
    tail, *early = call(
        early_kernel,
        (shape((8, CHANNELS + 2 * STATE), BF16),) + prepared,
        loads,
        in_specs=[ANY] * 7,
    )(*sources)
    halo = lax.ppermute(tail, ("y", "z", "core"), [(i, i + 1) for i in range(1, 2 * CHIPS - 1, 2)])
    (
        step, log_rows, log_columns, _, now, near_x, near_proj, _, end, tapx, tapp,
        xm, pm, sums, send,
    ) = call(
        state_kernel,
        prepared
        + (
            shape(whole, BF16),
            shape((TOKENS_LOCAL, 2 * STATE), BF16),
            shape((2, rows, HALF), F32),
            shape((rows, HALF), F32),
        ),
        loads,
        10**9,
        in_specs=[ANY] * 7 + [NEAR] * 11,
        input_output_aliases={7 + i: i for i in range(11)},
    )(*sources, *(near(value) for value in early))
    swap = [(0, 1), (1, 0)]
    other = lax.ppermute(send, "core", swap)
    small = [pltpu.VMEM((16, CHANNELS), F32), pltpu.VMEM((16, 2 * STATE), F32)]
    ranks = shape((8, HALF + STATE), BF16)
    own_rows, rows_send = call(first_kernel, (ranks, ranks), small)(
        near(halo), near(near_x), near(near_proj), near(end), near(tapx), near(tapp)
    )
    came_rows = lax.ppermute(rows_send, "core", [(0, 1)])
    message, first = call(
        join_kernel,
        (shape((CHIPS, 5, 2, 128), BF16), shape((STATE + 8, HALF), F32)),
        [pltpu.VMEM((16, HALF), F32), pltpu.VMEM((16, 2 * STATE), F32)],
    )(
        near(sums), near(other), near(near_x), near(near_proj), near(tapx), near(tapp),
        near(own_rows), near(came_rows),
    )
    gathered = lax.all_to_all(message, chips, 0, 0, tiled=True)
    entering = call(scan_kernel, shape((CHIPS, 8, 2, 128), BF16))(near(gathered))
    returned = lax.all_to_all(entering, chips, 0, 0, tiled=True)
    keep, give = call(
        enter_kernel, (shape((STATE, HALF), BF16), shape((STATE, HALF), BF16))
    )(near(returned), near(first))
    got = lax.ppermute(give, "core", swap)
    within, read, outer = call(
        within_kernel,
        (shape(whole, F32), shape((TOKENS_LOCAL, STATE), BF16), shape(whole, F32)),
        [pltpu.VMEM(whole, BF16), pltpu.VMEM((TOKENS_LOCAL, STATE), BF16)] + small,
        10**10,
    )(
        near(xm), near(pm), near(step), near(log_rows), near(log_columns), near(now),
        gate_inputs[0], near(halo), near(other), near(near_x), near(near_proj), near(tapx),
        near(tapp),
    )
    gated, square = call(
        gate_kernel, (shape((TOKENS_LOCAL, CHANNELS), F32), shape((2, 128), F32))
    )(near(keep), near(got), near(read), near(within), near(outer))
    squares = lax.all_gather(square, "head")
    out = call(
        norm_kernel,
        pltpu.HBM((TOKENS_LOCAL, CHANNELS), BF16),
        [pltpu.VMEM((TOKENS_LOCAL, CHANNELS), BF16), pltpu.SemaphoreType.DMA((8,))],
        out_specs=ANY,
    )(near(gated), near(squares), norm_gain[None])
    return out[None]


def solution(mesh):
    grid = Mesh(mesh.devices.reshape(8, 8, 2, 4), ("y", "z", "core", "head"))
    seq = ("y", "z", "core")
    return jax.shard_map(
        shards,
        mesh=grid,
        in_specs=(
            P(None, seq, "head"),
            P(None, seq, "head"),
            P(None, seq, None),
            P(None, seq, "head"),
            P("head"),
            P("head"),
            P(None, "head"),
            P(),
            P("head"),
        ),
        out_specs=P(None, seq, "head"),
        check_vma=False,
    )
```
